32 devices in a mesh: fluid: 8 (over z, y), grp: 4 (over x, core).
Axes of the slice: x: 2, y: 2, z: 4, core: 2. Of those that a mesh axis runs over, the one named last changes fastest.
Arguments:
- acoustic_modes: bfloat16 [262144, 400], P(('fluid', 'grp')), may hold values from -6 to 6
- shell_modes: bfloat16 [8192, 300], P('fluid'), may hold values from -0.0012207031 to 0.0012207031
- wet_counts: int32 [32], P(('fluid', 'grp')), may hold values from 1 to 2048, 26214 in all
- fluid_nodes: int32 [65536], P(('fluid', 'grp')), may hold values from 0 to 8191
- shell_nodes: int32 [65536], P(('fluid', 'grp')), may hold values from 0 to 1023
- wet_area: float32 [65536], P(('fluid', 'grp')), may hold values from 0.15 to 0.6
- shell_freq: float32 [300], replicated, may hold values from 1 to 2
- shell_loss: float32 [300], replicated, may hold values from 0.2 to 0.5
- cavity_freq: float32 [400], replicated, may hold values from 1 to 2
- cavity_loss: float32 [400], replicated, may hold values from 0.2 to 0.5
- freqs: float32 [64], replicated, may hold values from 0.7 to 2.2
- modal_force: float32 [300], replicated, may hold values from -1.5 to 1.5
- cavity_source: float32 [400], replicated, may hold values from -1.5 to 1.5
Outputs:
- pressure: bfloat16 [262144, 128], P(('fluid', 'grp'))
- modal_structure: float32 [2, 64, 300], P(None, 'grp')
The draws below stay inside these ranges and needn't reach their ends.
Inputs may be any that keep to these rules, and one draw needn't show every extreme that they name: `wet_counts`: slots 0 to count - 1 of a device's 2048 interface slots are live, the others are ignored. `fluid_nodes`: numbered within the device's own 8192 cavity rows. `shell_nodes`: numbered within the 1024 shell rows of the device's fluid index.
All inputs are finite; a program needn't handle non-finite values.
Results may differ from the reference program's by a relative error of at most 0.0055.
Values may be sent and summed in bfloat16 or wider, within the bound.
No kernel may reach another device: no remote copies, remote signals or barrier semaphores. Data moves between devices by JAX's collectives and lax.ppermute only.
A program may use at most 64 MiB of HBM per device.

```python
import math
import jax
import jax.numpy as jnp
import numpy as np
from jax import lax

MS = 300
MA = 400
F = 64
SECTIONS = 4
FD = 8192
SD = 1024
IF_MOST = 2048
FLUID_DOFS = 262144
SHELL_DOFS = 8192
SLOTS = 65536
N_FLUID = 8
N_GRP = 4


def place_ends(entries, stream_key, smallest, high):
    extent = entries.shape
    spot = [jax.random.randint(jax.random.fold_in(stream_key, axis), (), 0, extent[axis]) for axis in range(len(extent))]
    entries = entries.at[tuple(spot)].set(smallest)
    longest = extent.index(max(extent))
    spot[longest] = (spot[longest] + 1) % extent[longest]
    return entries.at[tuple(spot)].set(high)


def steps_of(rng, shape, shards, smallest, top_value):
    def one(dim, parts):
        draws = jax.random.uniform(jax.random.fold_in(jax.random.fold_in(rng, 6), dim), (parts,), jnp.float32, smallest / len(shards), top_value / len(shards))
        return jnp.repeat(jnp.exp(draws), shape[dim] // parts).reshape((-1,) + (1,) * (len(shape) - dim - 1))

    level = one(*shards[0])
    for cut in shards[1:]:
        level = level * one(*cut)
    return level


def split_up(amount, total, limit, lean):
    weights = [(1 << 20) // math.isqrt(rank ** lean) + 1 for rank in range(2, amount + 1)]
    spare, counts = total - limit - (amount - 1), [1] * (amount - 1)
    while spare > 0:
        movable = [i for i in range(amount - 1) if counts[i] < limit]
        mass, budget = sum([weights[i] for i in movable]), spare
        for i in movable:
            addition = min(limit - counts[i], max(1, budget * weights[i] // mass), spare)
            counts[i] = counts[i] + addition
            spare = spare - addition
    return np.array([limit] + counts)


def ragged(own_key, number_of, total, most, lean):
    if number_of == 2:
        one = jax.random.randint(own_key, (), max(1, total - most), min(most, total - 1) + 1)
        return jnp.stack([one, total - one])
    sizes = jnp.asarray(split_up(number_of, total, most, lean), jnp.int32)
    twos = (number_of - 1) // 2
    donor, receiver = sizes[1:1 + 2 * twos:2], sizes[2:2 + 2 * twos:2]
    slack = jnp.minimum(donor - 1, most - receiver)
    passed = jax.random.randint(jax.random.fold_in(own_key, 1), (twos,), 0, 1 << 20) % (slack + 1)
    sizes = sizes.at[1:1 + 2 * twos:2].set(donor - passed).at[2:2 + 2 * twos:2].set(receiver + passed)
    return sizes[jax.random.permutation(jax.random.fold_in(own_key, 2), number_of)]


def centred(key, extent, scale, reach, split=(), held_as=jnp.bfloat16):
    entries = scale * jax.random.normal(key, extent, jnp.float32)
    if split:
        entries = entries * steps_of(key, extent, split, -0.22, 0.18)
    return jnp.clip(entries, -reach, reach).astype(held_as)


def setup_inputs(seed: int = 0) -> dict:
    splits = jax.random.split(jax.random.key(seed), 14)
    acoustic_modes = centred(splits[0], (FLUID_DOFS, MA), 1.0, 6.0, ((0, 32),))
    shell_modes = centred(splits[1], (SHELL_DOFS, MS), (N_FLUID * N_GRP * IF_MOST * MA) ** -0.5, 0.0012207031, ((0, 8),))
    wet_counts = ragged(splits[2], N_FLUID * N_GRP, N_FLUID * N_GRP * IF_MOST * 2 // 5, IF_MOST, 2).astype(jnp.int32)
    fluid_nodes = place_ends(jax.random.randint(splits[3], (SLOTS,), 0, FD), jax.random.fold_in(splits[3], 1), 0, FD - 1).astype(jnp.int32)
    shell_nodes = place_ends(jax.random.randint(splits[4], (SLOTS,), 0, SD), jax.random.fold_in(splits[4], 1), 0, SD - 1).astype(jnp.int32)
    wet_area = jnp.clip(jnp.exp(math.log(0.6) - 1.3862944 * jax.random.uniform(splits[5], (SLOTS,), jnp.float32) ** steps_of(splits[5], (SLOTS,), ((0, 32),), -0.2, 0.2)), 0.15, 0.6)
    shell_freq = jnp.clip(jnp.exp(jax.random.uniform(splits[6], (MS,), jnp.float32, math.log(1.0), math.log(2.0))), 1.0, 2.0)
    shell_loss = jnp.clip(jnp.exp(jax.random.uniform(splits[7], (MS,), jnp.float32, math.log(0.2), math.log(0.5))), 0.2, 0.5)
    cavity_freq = jnp.clip(jnp.exp(jax.random.uniform(splits[8], (MA,), jnp.float32, math.log(1.0), math.log(2.0))), 1.0, 2.0)
    cavity_loss = jnp.clip(jnp.exp(jax.random.uniform(splits[9], (MA,), jnp.float32, math.log(0.2), math.log(0.5))), 0.2, 0.5)
    freqs = jnp.clip(jax.random.uniform(splits[10], (F,), jnp.float32, 0.7, 2.2), 0.7, 2.2)
    modal_force = centred(splits[11], (MS,), 0.25, 1.5, (), jnp.float32)
    cavity_source = centred(splits[12], (MA,), 0.25, 1.5, (), jnp.float32)
    return dict(acoustic_modes=acoustic_modes, shell_modes=shell_modes, wet_counts=wet_counts, fluid_nodes=fluid_nodes, shell_nodes=shell_nodes, wet_area=wet_area, shell_freq=shell_freq, shell_loss=shell_loss, cavity_freq=cavity_freq, cavity_loss=cavity_loss, freqs=freqs, modal_force=modal_force, cavity_source=cavity_source)


HIGH = lax.Precision.HIGHEST


def divide_complex(real_part, imag_part, denom_real, denom_imag):
    scale = denom_real * denom_real + denom_imag * denom_imag
    return ((real_part * denom_real + imag_part * denom_imag) / scale,
            (imag_part * denom_real - real_part * denom_imag) / scale)


def modal_terms(omega, loss, freqs):
    stiff = omega * omega
    real_part = stiff[None, :] - (freqs * freqs)[:, None]
    imag_part = jnp.broadcast_to((loss * stiff)[None, :], real_part.shape)
    return real_part, imag_part


def reference(acoustic_modes, shell_modes, wet_counts, fluid_nodes, shell_nodes, wet_area, shell_freq, shell_loss, cavity_freq, cavity_loss, freqs, modal_force, cavity_source):
    devices = N_FLUID * N_GRP
    fluid_blocks = acoustic_modes.reshape(devices, FD, MA)
    shell_blocks = shell_modes.reshape(N_FLUID, SD, MS)

    def accumulate(carry, device):
        fluid_part = lax.dynamic_index_in_dim(fluid_blocks, device, 0, keepdims=False)
        shell_part = lax.dynamic_index_in_dim(shell_blocks, device // N_GRP, 0, keepdims=False)
        start = (device * IF_MOST).astype(jnp.int32)
        fluid_pick = lax.dynamic_slice_in_dim(fluid_nodes, start, IF_MOST)
        shell_pick = lax.dynamic_slice_in_dim(shell_nodes, start, IF_MOST)
        area = lax.dynamic_slice_in_dim(wet_area, start, IF_MOST)
        count = lax.dynamic_index_in_dim(wet_counts, device, 0, keepdims=False)
        live = (jnp.arange(IF_MOST, dtype=jnp.int32) < count).astype(jnp.float32)
        wet = (area[:, None] * fluid_part[fluid_pick].astype(jnp.float32) * live[:, None]).astype(jnp.bfloat16)
        shell_rows = shell_part[shell_pick]
        carry = carry + jnp.dot(shell_rows.astype(jnp.float32).T, wet.astype(jnp.float32), precision=HIGH)
        return carry, None

    coupling, unused = lax.scan(accumulate, jnp.zeros((MS, MA), jnp.float32), jnp.arange(devices, dtype=jnp.int32))

    ds_re, ds_im = modal_terms(shell_freq, shell_loss, freqs)
    da_re, da_im = modal_terms(cavity_freq, cavity_loss, freqs)
    free_re, free_im = divide_complex(jnp.broadcast_to(cavity_source[None, :], da_re.shape), jnp.zeros_like(da_re), da_re, da_im)
    squared = (freqs * freqs)[:, None]
    coupled_re = jnp.zeros_like(free_re)
    coupled_im = jnp.zeros_like(free_im)
    for section in range(SECTIONS):
        amounts = jnp.concatenate([free_re + coupled_re, free_im + coupled_im], 0)
        loads = jnp.dot(amounts, coupling.T, precision=HIGH)
        struct_re, struct_im = divide_complex(modal_force[None, :] + loads[:F], loads[F:], ds_re, ds_im)
        back = jnp.dot(jnp.concatenate([struct_re, struct_im], 0), coupling, precision=HIGH)
        coupled_re, coupled_im = divide_complex(squared * back[:F], squared * back[F:], da_re, da_im)
    modal_structure = jnp.stack([struct_re, struct_im])

    free_amps = lax.optimization_barrier(jnp.concatenate([free_re, free_im], 0).astype(jnp.bfloat16))
    coupled_amps = lax.optimization_barrier(jnp.concatenate([coupled_re, coupled_im], 0).astype(jnp.bfloat16))
    amplitudes = free_amps.astype(jnp.float32) + coupled_amps.astype(jnp.float32)

    def recover(block):
        return jnp.dot(block.astype(jnp.float32), amplitudes.T, precision=HIGH).astype(jnp.bfloat16)

    pressure = lax.map(recover, fluid_blocks).reshape(devices * FD, 2 * F)
    return pressure, modal_structure
```

```python
import functools

import jax
import jax.numpy as jnp
from jax import lax
from jax.experimental import pallas as pl
from jax.experimental.pallas import tpu as pltpu
from jax.sharding import PartitionSpec as P

SECTIONS = 4
LANES = 128
SLOT_BLOCK = 256
F32 = jnp.float32
BF16 = jnp.bfloat16


def ceil_to(value, step):
    return (value + step - 1) // step * step


def divide_complex(real_part, imag_part, denom_real, denom_imag):
    scale = 1.0 / (denom_real * denom_real + denom_imag * denom_imag)
    return (
        (real_part * denom_real + imag_part * denom_imag) * scale,
        (imag_part * denom_real - real_part * denom_imag) * scale,
    )


class Packing:
    def __init__(self, rows, columns, parts):
        self.rows, self.columns = rows, columns
        self.padded = ceil_to(rows, 8)
        self.full, self.tail = columns // LANES, columns % LANES
        self.pieces = LANES // self.tail if self.tail else 1
        self.group = ceil_to(-(-self.padded // self.pieces), 8) if self.tail else 0
        self.total = ceil_to(self.padded * self.full + self.group, 16 * parts)

    def store(self, out_ref, matrix):
        for j in range(self.full):
            out_ref[pl.ds(j * self.padded, self.padded), :] = matrix[
                :, j * LANES : (j + 1) * LANES
            ].astype(out_ref.dtype)
        first = self.full * self.padded
        if self.tail:
            rest = matrix[:, self.full * LANES :]
            packed = None
            for piece in range(self.pieces):
                low = piece * self.group
                high = min(low + self.group, self.padded)
                if low >= high:
                    break
                part = rest[low:high]
                if high - low < self.group:
                    part = jnp.concatenate(
                        [part, jnp.zeros((self.group - (high - low), LANES), part.dtype)], 0
                    )
                if piece:
                    part = pltpu.roll(part, piece * self.tail, 1)
                packed = part if packed is None else packed + part
            out_ref[pl.ds(first, self.group), :] = packed.astype(out_ref.dtype)
            first += self.group
        if first < self.total:
            out_ref[pl.ds(first, self.total - first), :] = jnp.zeros(
                (self.total - first, LANES), out_ref.dtype
            )

    def load(self, values):
        tiles = [values[j * self.padded : (j + 1) * self.padded] for j in range(self.full)]
        if self.tail:
            first = self.full * self.padded
            packed = values[first : first + self.group]
            lane = lax.broadcasted_iota(jnp.int32, packed.shape, 1)
            parts = []
            for piece in range(self.pieces):
                low = piece * self.group
                high = min(low + self.group, self.padded)
                if low >= high:
                    break
                part = pltpu.roll(packed, (LANES - piece * self.tail) % LANES, 1) if piece else packed
                part = jnp.where(lane < self.tail, part, 0.0)
                parts.append(part[: high - low])
            tiles.append(jnp.concatenate(parts, 0))
        return jnp.concatenate(tiles, 1)


def couple_kernel(
    packing,
    count_ref,
    nodes_ref,
    modes_ref,
    shell_ref,
    shell_nodes_ref,
    area_ref,
    out_ref,
    flat_ref,
    table,
    picked,
):
    step = pl.program_id(0)
    cavity, width = modes_ref.shape
    pad = table.shape[1] * LANES
    piece = 256

    row = lax.broadcasted_iota(jnp.int32, (piece, piece), 0)
    col = lax.broadcasted_iota(jnp.int32, (piece, piece), 1)
    unit = (row == col).astype(BF16)
    for part in range(width // piece):
        block = modes_ref[:, part * piece : (part + 1) * piece]
        turned = lax.dot_general(
            unit, block, (((1,), (1,)), ((), ())), preferred_element_type=F32
        )
        flat_ref[pl.ds(part * piece, piece), :] = turned.astype(BF16)
        turned = jnp.concatenate([turned, jnp.zeros((piece, pad - cavity), F32)], 1)
        at = pl.multiple_of(step * width + part * piece, piece)
        for j in range(table.shape[1]):
            table[pl.ds(at, piece), j, :] = turned[:, j * LANES : (j + 1) * LANES]

    @pl.when(step == pl.num_programs(0) - 1)
    def _():
        count = count_ref[0]
        shell = shell_ref[...]
        nodes, modes = shell.shape[1], shell.shape[0]

        def add_block(number, total):
            base = pl.multiple_of(number * SLOT_BLOCK, SLOT_BLOCK)

            def pick(group, _):
                first = group * 16
                for slot in range(16):
                    picked[first + slot] = table[nodes_ref[base + first + slot]]
                return 0

            lax.fori_loop(0, SLOT_BLOCK // 16, pick, 0)
            rows = jnp.concatenate(
                [picked[:, j, :] for j in range(table.shape[1])], 1
            ).astype(BF16)
            ids = shell_nodes_ref[:, pl.ds(base, SLOT_BLOCK)]
            chosen = lax.broadcasted_iota(jnp.int32, (nodes, SLOT_BLOCK), 0) == ids
            shell_rows = jnp.dot(shell, chosen.astype(BF16), preferred_element_type=F32)
            slot = base + lax.broadcasted_iota(jnp.int32, (1, SLOT_BLOCK), 1)
            weight = jnp.where(slot < count, area_ref[:, pl.ds(base, SLOT_BLOCK)], 0.0)
            scaled = (shell_rows * weight).astype(BF16)
            return total + jnp.dot(scaled, rows, preferred_element_type=F32)

        total = lax.fori_loop(
            0,
            (count + SLOT_BLOCK - 1) // SLOT_BLOCK,
            add_block,
            jnp.zeros((modes, pad), F32),
        )
        total = jnp.concatenate(
            [total, jnp.zeros((packing.padded - modes, pad), F32)], 0
        )
        packing.store(out_ref, total)


def couple(packing, count, nodes, modes_t, shell_t, shell_nodes, area, width):
    cavity, dofs = modes_t.shape
    tiles = -(-cavity // LANES)
    smem = pl.BlockSpec(memory_space=pltpu.SMEM)
    whole = lambda a: pl.BlockSpec(a.shape, lambda i: (0, 0))
    return pl.pallas_call(
        functools.partial(couple_kernel, packing),
        grid=(dofs // width,),
        in_specs=[
            smem,
            smem,
            pl.BlockSpec((cavity, width), lambda i: (0, i)),
            whole(shell_t),
            whole(shell_nodes),
            whole(area),
        ],
        out_specs=[
            pl.BlockSpec((packing.total, LANES), lambda i: (0, 0)),
            pl.BlockSpec((width, cavity), lambda i: (i, 0)),
        ],
        out_shape=[
            jax.ShapeDtypeStruct((packing.total, LANES), BF16),
            jax.ShapeDtypeStruct((dofs, cavity), BF16),
        ],
        scratch_shapes=[
            pltpu.VMEM((dofs, tiles, LANES), F32),
            pltpu.VMEM((SLOT_BLOCK, tiles, LANES), F32),
        ],
        name="couple",
    )(count, nodes, modes_t, shell_t, shell_nodes, area)


def split_dot(values, matrix, dims):
    rows = values.shape[0]
    high = values.astype(BF16)
    low = (values - high.astype(F32)).astype(BF16)
    both = lax.dot_general(
        jnp.concatenate([high, low], 0), matrix, (dims, ((), ())), preferred_element_type=F32
    )
    return both[:rows] + both[rows:]


def recover_kernel(
    packing,
    member_ref,
    coupling_ref,
    shell_freq_ref,
    shell_loss_ref,
    cavity_freq_ref,
    cavity_loss_ref,
    freqs_ref,
    force_ref,
    source_ref,
    flat_ref,
    pressure_ref,
    struct_ref,
    weights,
    structure,
):
    count = freqs_ref.shape[1]
    own = struct_ref.shape[1]

    @pl.when(pl.program_id(0) == 0)
    def _():
        matrix = packing.load(coupling_ref[...].astype(F32))
        matrix = matrix[: packing.rows, : packing.columns].astype(BF16)
        row = lax.broadcasted_iota(jnp.int32, (count, count), 0)
        col = lax.broadcasted_iota(jnp.int32, (count, count), 1)
        freqs = jnp.sum(jnp.where(row == col, freqs_ref[...], 0.0), 1, keepdims=True)
        squared = freqs * freqs

        def terms(freq_ref, loss_ref):
            stiff = freq_ref[...] * freq_ref[...]
            real_part = stiff - squared
            imag_part = jnp.broadcast_to(loss_ref[...] * stiff, real_part.shape)
            scale = 1.0 / (real_part * real_part + imag_part * imag_part)
            return real_part * scale, imag_part * scale

        ds_re, ds_im = terms(shell_freq_ref, shell_loss_ref)
        da_re, da_im = terms(cavity_freq_ref, cavity_loss_ref)
        free_re = source_ref[...] * da_re
        free_im = -source_ref[...] * da_im
        wa_re, wa_im = squared * da_re, squared * da_im
        free = jnp.concatenate([free_re, free_im], 0)
        amounts = free
        force = force_ref[...]
        for section in range(SECTIONS):
            loads = split_dot(amounts, matrix, ((1,), (1,)))
            load_re, load_im = force + loads[:count], loads[count:]
            struct_re = load_re * ds_re + load_im * ds_im
            struct_im = load_im * ds_re - load_re * ds_im
            back = split_dot(jnp.concatenate([struct_re, struct_im], 0), matrix, ((1,), (0,)))
            back_re, back_im = back[:count], back[count:]
            coupled = jnp.concatenate(
                [back_re * wa_re + back_im * wa_im, back_im * wa_re - back_re * wa_im], 0
            )
            amounts = free + coupled
        weights[...] = jnp.concatenate([free.astype(BF16), coupled.astype(BF16)], 0)
        structure[0] = struct_re
        structure[1] = struct_im
        start = pl.multiple_of(member_ref[0] * own, own)
        struct_ref[...] = structure[:, pl.ds(start, own), :]

    both = lax.dot_general(
        flat_ref[...], weights[...], (((1,), (1,)), ((), ())), preferred_element_type=F32
    )
    pressure_ref[...] = (both[:, : 2 * count] + both[:, 2 * count :]).astype(BF16)


def recover(packing, groups, member, coupling, vectors, flat, width):
    dofs, cavity = flat.shape
    shell_freq, shell_loss, cavity_freq, cavity_loss, freqs, force, source = vectors
    count = freqs.shape[1]
    whole = lambda a: pl.BlockSpec(a.shape, lambda i: (0, 0))
    return pl.pallas_call(
        functools.partial(recover_kernel, packing),
        grid=(dofs // width,),
        in_specs=[pl.BlockSpec(memory_space=pltpu.SMEM), whole(coupling)]
        + [whole(v) for v in vectors]
        + [pl.BlockSpec((width, cavity), lambda i: (i, 0))],
        out_specs=[
            pl.BlockSpec((width, 2 * count), lambda i: (i, 0)),
            pl.BlockSpec((2, count // groups, packing.rows), lambda i: (0, 0, 0)),
        ],
        out_shape=[
            jax.ShapeDtypeStruct((dofs, 2 * count), BF16),
            jax.ShapeDtypeStruct((2, count // groups, packing.rows), F32),
        ],
        scratch_shapes=[
            pltpu.VMEM((4 * count, cavity), BF16),
            pltpu.VMEM((2, count, packing.rows), F32),
        ],
        name="recover",
    )(member, coupling, *vectors, flat)


def partner(axis, bit):
    return [(i, i ^ bit) for i in range(lax.axis_size(axis))]


def halve(values, axis, bit):
    half = values.shape[0] // 2
    upper = (lax.axis_index(axis) & bit) != 0
    sent = jnp.where(upper, values[:half], values[half:])
    kept = jnp.where(upper, values[half:], values[:half])
    got = lax.ppermute(sent.astype(BF16), axis, partner(axis, bit))
    return kept.astype(F32) + got.astype(F32)


def exchange(values, axis, bit):
    mine = values.astype(BF16)
    return mine.astype(F32) + lax.ppermute(mine, axis, partner(axis, bit)).astype(F32)


def rejoin(values, axis, bit):
    mine = values.astype(BF16)
    upper = (lax.axis_index(axis) & bit) != 0
    got = lax.ppermute(mine, axis, partner(axis, bit))
    return jnp.concatenate([jnp.where(upper, got, mine), jnp.where(upper, mine, got)], 0)


def bits_of(size):
    return [1 << k for k in range(size.bit_length() - 1)]


def sum_everywhere(values):
    group_bits = bits_of(lax.axis_size("grp"))
    for bit in group_bits:
        values = halve(values, "grp", bit)
    for bit in bits_of(lax.axis_size("fluid")):
        values = exchange(values, "fluid", bit)
    for bit in reversed(group_bits):
        values = rejoin(values, "grp", bit)
    return values


def on_device(
    acoustic_modes,
    shell_modes,
    wet_counts,
    fluid_nodes,
    shell_nodes,
    wet_area,
    shell_freq,
    shell_loss,
    cavity_freq,
    cavity_loss,
    freqs,
    modal_force,
    cavity_source,
):
    groups = lax.axis_size("grp")
    member = lax.axis_index("grp").astype(jnp.int32).reshape(1)
    packing = Packing(shell_modes.shape[1], acoustic_modes.shape[1], groups)
    partial_sum, flat = couple(
        packing,
        wet_counts,
        fluid_nodes,
        acoustic_modes.T,
        shell_modes.T,
        shell_nodes[None, :],
        wet_area[None, :],
        512,
    )
    coupling = sum_everywhere(partial_sum)
    vectors = [
        v[None, :]
        for v in (
            shell_freq,
            shell_loss,
            cavity_freq,
            cavity_loss,
            freqs,
            modal_force,
            cavity_source,
        )
    ]
    return tuple(recover(packing, groups, member, coupling, vectors, flat, 1024))


def solution(mesh):
    assert mesh.shape["fluid"] & (mesh.shape["fluid"] - 1) == 0
    assert mesh.shape["grp"] & (mesh.shape["grp"] - 1) == 0
    placed = (
        P(("fluid", "grp"), None),
        P("fluid", None),
        P(("fluid", "grp")),
        P(("fluid", "grp")),
        P(("fluid", "grp")),
        P(("fluid", "grp")),
        P(),
        P(),
        P(),
        P(),
        P(),
        P(),
        P(),
    )
    return jax.shard_map(
        on_device,
        mesh=mesh,
        in_specs=placed,
        out_specs=(P(("fluid", "grp"), None), P(None, "grp", None)),
        check_vma=False,
    )
```
